256 devices in a mesh: grp: 8 (over x, core), mem: 32 (over z, y).
Axes of the slice: x: 4, y: 4, z: 8, core: 2. Of those that a mesh axis runs over, the one named last changes fastest.
Arguments:
- slab: float32 [2048, 16384], P('mem', 'grp'), may hold values from 0 to 32, as said below
- tiles: float32 [8192, 16384], P('grp', 'mem'), may hold values from 0 to 1.05, as said below
- slot_rows: int32 [16, 32], P('grp'), may hold values from -1 to 3, as said below
Outputs:
- clustered: float32 [2048, 16384], P('grp', 'mem')
The draws below stay inside these ranges and needn't reach their ends.
Inputs may be any that keep to these rules, and one draw needn't show every extreme that they name: For each group g and block column m, the used slots h (slot_rows[g * 2 + h, m] >= 0) come first and name distinct block rows of the group; unused slots hold -1. Each block column has at least one used slot in every group, and in every draw some group and block column has all 2 slots used. Entries are nonnegative, positive in the tiles of used slots, and zero in the tiles of unused slots. `slab`: entries are positive.
All inputs are finite; a program needn't handle non-finite values.
Results may differ from the reference program's by a relative error of at most 0.0003.
Values sent between devices are 32-bit elements; how exact they have to be, the bound alone decides.
A program may use at most 64 MiB of HBM per device.

```python
import jax
import jax.numpy as jnp
from jax import lax

TILE = 512
HELD = 2
GROUPS = 8
MEMBERS = 32
GROUP_BLOCKS = 4
NCOLS = 16384
WROWS = 2048


def slot_layout(key):
    anchor = jax.random.fold_in(key, 7)
    device_count = GROUPS * MEMBERS
    device_keys = jax.random.split(anchor, device_count)
    orders = jax.vmap(lambda subkey: jax.random.permutation(subkey, GROUP_BLOCKS)[:HELD])(device_keys)
    counts = jax.random.randint(jax.random.fold_in(anchor, 1), (device_count,), 1, HELD + 1)
    chosen_full = jax.random.randint(jax.random.fold_in(anchor, 2), (), 0, device_count)
    counts = jnp.where(jnp.arange(device_count) == chosen_full, HELD, counts)
    slot_ids = jnp.arange(HELD)[None, :]
    row_table = jnp.where(slot_ids < counts[:, None], orders, -1)
    row_table = row_table.reshape(GROUPS, MEMBERS, HELD).transpose(0, 2, 1).reshape(GROUPS * HELD, MEMBERS)
    return row_table.astype(jnp.int32)


def draw_slot_rows(key, part):
    return slot_layout(key)


def draw_tiles(key, part):
    layout = slot_layout(key)
    filled = (layout >= 0).astype(jnp.float32)
    values = jax.random.uniform(jax.random.fold_in(key, 11), (GROUPS * HELD * TILE, NCOLS), jnp.float32)
    entries = jnp.exp(jnp.log(0.01) + values * jnp.log(100.0))
    expand_mask = jnp.repeat(jnp.repeat(filled, TILE, axis=0), TILE, axis=1)
    return entries * expand_mask


def draw_slab(key, part):
    values = jax.random.uniform(jax.random.fold_in(key, 21), (WROWS, NCOLS), jnp.float32)
    scale_draw = jax.random.uniform(jax.random.fold_in(key, 22), (WROWS, 1), jnp.float32)
    position = jnp.arange(WROWS, dtype=jnp.float32)[:, None] / WROWS
    row_scale = jnp.exp(scale_draw * jnp.log(10.0)) * jnp.exp(position * jnp.log(3.0))
    entries = jnp.exp(jnp.log(0.01) + values * jnp.log(100.0))
    return entries * row_scale


def setup_inputs(seed: int = 0) -> dict:
    key_list = jax.random.split(jax.random.key(seed), 4)
    return {
        "slab": draw_slab(jax.random.fold_in(key_list[3], 71), 0),
        "tiles": draw_tiles(jax.random.fold_in(key_list[3], 71), 0),
        "slot_rows": draw_slot_rows(jax.random.fold_in(key_list[3], 71), 0),
    }


def column_block(member, slab, tiles, slot_rows):
    tile_column = lax.dynamic_slice_in_dim(tiles, member * TILE, TILE, 1).reshape(GROUPS * HELD, TILE, TILE)
    local_rows = lax.dynamic_index_in_dim(slot_rows, member, axis=1, keepdims=False)
    group_ids = jnp.repeat(jnp.arange(GROUPS, dtype=jnp.int32), HELD)
    block_ids = (group_ids * GROUP_BLOCKS + jnp.maximum(local_rows, 0)).astype(jnp.int32)
    slab_blocks = slab.reshape(WROWS, MEMBERS, TILE)
    chosen = jnp.take(slab_blocks, block_ids, axis=1)
    return jnp.einsum("wst,stu->wu", chosen, tile_column, precision=lax.Precision.HIGHEST)


def reference(slab, tiles, slot_rows):
    members = jnp.arange(MEMBERS, dtype=jnp.int32)
    blocks = lax.map(lambda member: column_block(member, slab, tiles, slot_rows), members)
    expanded = jnp.transpose(blocks, (1, 0, 2)).reshape(WROWS, NCOLS)
    inflated = expanded * expanded
    column_means = jnp.sum(inflated, axis=0) / WROWS
    return inflated / column_means
```

```python
import functools

import jax
import jax.numpy as jnp
from jax import lax
from jax.experimental import pallas as pl
from jax.experimental.pallas import tpu as pltpu
from jax.sharding import PartitionSpec as P

MESH = pl.DeviceIdType.MESH
F32 = jnp.float32
BF16 = jnp.bfloat16

TILE = 512
ROWS = 64
KCOLS = 2048
HALF = 1024
ZN, YN, XN, GN = 8, 4, 4, 8
WROWS = 2048

UP, DOWN, ACROSS = 0, 1, 2
NA, NB = 0, 1
LO, HI = 0, 1


def body(
    slab, tiles, slot_rows, out,
    rows, tile_buf, thi, tlo, xhi, xlo, part, sib, csum, mid, dst, ybuf, fin, stage, sq, sq_all,
    load_sem, gsend, grecv, tsend, trecv, dsend, drecv, xsend, mrecv, rrecv, ysend, yrecv, qsend, qrecv,
):
    g = lax.axis_index("grp")
    m = lax.axis_index("mem")
    x, core = g // 2, g % 2
    z, y = m // YN, m % YN
    pair_y = y + 1 - 2 * (y % 2)
    m_up = ((z + 1) % ZN) * YN + y
    m_down = ((z + ZN - 1) % ZN) * YN + y
    m_across = z * YN + (3 - y)
    m_pair = z * YN + pair_y
    g_sib = x * 2 + (1 - core)

    def dev(gi, mi):
        return {"grp": gi, "mem": mi}

    load_slab = pltpu.make_async_copy(slab, rows.at[NA, 0], load_sem.at[0])
    load_tiles = pltpu.make_async_copy(tiles, tile_buf.at[0], load_sem.at[1])
    load_slab.start()
    load_tiles.start()

    barrier = pltpu.get_barrier_semaphore()
    for mi in (m_up, m_down, m_across, m_pair):
        pl.semaphore_signal(barrier, inc=1, device_id=dev(g, mi), device_id_type=MESH)
    for d in range(1, GN):
        pl.semaphore_signal(barrier, inc=1, device_id=dev((g + d) % GN, m), device_id_type=MESH)
    pl.semaphore_wait(barrier, 4 + GN - 1)

    started = []

    def piece(w, s, h):
        return rows.at[w, s, :, pl.ds(h * HALF, HALF)]

    def move(way, w, s, h):
        if way == ACROSS:
            target, tw, ts = m_across, NB, s
        elif way == UP:
            target, tw, ts = m_up, w, s + 1
        else:
            target, tw, ts = m_down, w, (s + 7) % 8
        copy = pltpu.make_async_remote_copy(
            src_ref=piece(w, s, h), dst_ref=piece(tw, ts, h),
            send_sem=gsend.at[len(started)], recv_sem=grecv.at[tw, ts, h],
            device_id=dev(g, target), device_id_type=MESH,
        )
        copy.start()
        started.append(copy)

    def split(w, s, h):
        for b in range(2):
            block = s * 4 + h * 2 + b
            v = rows[w, s, :, pl.ds(h * HALF + b * TILE, TILE)]
            top = v.astype(BF16)
            xhi[block, pl.ds(w * ROWS, ROWS), :] = top
            xlo[block, pl.ds(w * ROWS, ROWS), :] = (v - top.astype(F32)).astype(BF16)

    def arrive(w, s, h):
        pltpu.make_async_remote_copy(
            src_ref=piece(w, s, h), dst_ref=piece(w, s, h),
            send_sem=gsend.at[0], recv_sem=grecv.at[w, s, h],
            device_id=dev(g, m_up), device_id_type=MESH,
        ).wait_recv()

    tile_copies = [
        pltpu.make_async_remote_copy(
            src_ref=tile_buf.at[0, pl.ds(h * TILE, TILE)], dst_ref=tile_buf.at[1, pl.ds(h * TILE, TILE)],
            send_sem=tsend.at[h], recv_sem=trecv.at[h],
            device_id=dev(g, m_pair), device_id_type=MESH,
        )
        for h in range(2)
    ]

    def split_tile(p, h):
        def step(i, carry):
            r = pl.multiple_of(i * 64, 64)
            v = tile_buf[p, pl.ds(h * TILE + r, 64), :]
            top = v.astype(BF16)
            thi[p * 2 + h, pl.ds(r, 64), :] = top
            tlo[p * 2 + h, pl.ds(r, 64), :] = (v - top.astype(F32)).astype(BF16)
            return carry
        lax.fori_loop(0, TILE // 64, step, 0)

    def product(s, p):
        member = m if p == 0 else m_pair
        u = s * 2 + p
        total = None
        for h in range(2):
            block = s * 4 + jnp.maximum(slot_rows[h, member], 0)
            a, b = xhi[block], xlo[block]
            c, d = thi[p * 2 + h], tlo[p * 2 + h]
            term = (
                jnp.dot(a, d, preferred_element_type=F32)
                + jnp.dot(b, c, preferred_element_type=F32)
                + jnp.dot(a, c, preferred_element_type=F32)
            )
            total = term if total is None else total + term
        part[u] = total.reshape(2, ROWS, TILE)
        sibling(u).start()

    def sibling(u):
        return pltpu.make_async_remote_copy(
            src_ref=part.at[u, 1 - core], dst_ref=sib.at[u],
            send_sem=dsend.at[u], recv_sem=drecv.at[u],
            device_id=dev(g_sib, m), device_id_type=MESH,
        )

    def place(s):
        zt = (z - s + ZN) % ZN
        xt, ct = zt // 2, zt % 2
        return xt, ct, (xt - x + XN) % XN

    def to_mid(u):
        xm = (x + 1 + 2 * core) % XN
        return pltpu.make_async_remote_copy(
            src_ref=csum.at[u], dst_ref=mid.at[u],
            send_sem=xsend.at[u], recv_sem=mrecv.at[u],
            device_id=dev(xm * 2 + core, m), device_id_type=MESH,
        )

    def to_dst(u, s, p):
        xt, ct, dx = place(s)
        side = jnp.where(dx == 1, 0, jnp.where(dx == 0, 1, 2))
        slot = p * 6 + side * 2 + core
        return pltpu.make_async_remote_copy(
            src_ref=csum.at[u], dst_ref=dst.at[slot],
            send_sem=xsend.at[u], recv_sem=rrecv.at[slot],
            device_id=dev(xt * 2 + ct, m), device_id_type=MESH,
        )

    def is_mid(dx):
        return ((dx == 1) & (core == 0)) | ((dx == 3) & (core == 1))

    def chip_sum(s, p):
        u = s * 2 + p
        xt, ct, dx = place(s)
        sibling(u).wait_recv()
        csum[u] = part[u, core] + sib[u]

        @pl.when(dx == 2)
        def _():
            to_mid(u).start()

        @pl.when(((dx == 0) & (ct != core)) | ((dx == 1) & (core == 1)) | ((dx == 3) & (core == 0)))
        def _():
            to_dst(u, s, p).start()

    def middle_sum(s, p):
        u = s * 2 + p
        xt, ct, dx = place(s)

        @pl.when(is_mid(dx))
        def _():
            to_mid(u).wait_recv()
            csum[u] = csum[u] + mid[u]
            to_dst(u, s, p).start()

    def finish(units):
        for s, p in units:
            chip_sum(s, p)
        for s, p in units:
            middle_sum(s, p)

    load_slab.wait()
    for h in (LO, HI):
        move(UP, NA, 0, h)
        move(DOWN, NA, 0, h)
        move(ACROSS, NA, 0, h)
    load_tiles.wait()
    for copy in tile_copies:
        copy.start()
    for h in (LO, HI):
        split(NA, 0, h)
    for h in range(2):
        split_tile(0, h)

    def arrive_near(h, s_up, s_down):
        arrive(NA, s_up, h)
        move(UP, NA, s_up, h)
        arrive(NA, s_down, h)
        move(DOWN, NA, s_down, h)

    for h in (LO, HI):
        arrive_near(h, 1, 7)
        move(ACROSS, NA, 1, h)
        move(ACROSS, NA, 7, h)
        split(NA, 1, h)
        split(NA, 7, h)
        arrive(NB, 0, h)
        split(NB, 0, h)
    product(0, 0)
    arrive_near(LO, 2, 6)
    arrive(NB, 1, LO)
    move(UP, NB, 1, LO)
    split(NA, 2, LO)
    split(NA, 6, LO)
    split(NB, 1, LO)
    arrive_near(HI, 2, 6)
    move(ACROSS, NA, 2, HI)
    arrive(NB, 7, LO)
    move(DOWN, NB, 7, LO)
    split(NA, 2, HI)
    split(NA, 6, HI)
    split(NB, 7, LO)
    finish([(0, 0)])
    arrive(NA, 3, LO)
    arrive(NA, 5, LO)
    split(NA, 3, LO)
    split(NA, 5, LO)
    arrive(NB, 1, HI)
    split(NB, 1, HI)
    product(1, 0)
    arrive(NB, 2, LO)
    move(UP, NB, 2, LO)
    move(UP, NA, 3, LO)
    arrive(NB, 6, LO)
    move(DOWN, NB, 6, LO)
    split(NB, 2, LO)
    split(NB, 6, LO)
    arrive(NB, 7, HI)
    split(NB, 7, HI)
    product(7, 0)
    finish([(1, 0)])
    arrive(NA, 3, HI)
    arrive(NA, 5, HI)
    move(ACROSS, NA, 5, HI)
    move(DOWN, NA, 5, HI)
    move(ACROSS, NA, 3, HI)
    move(ACROSS, NA, 6, HI)
    split(NA, 3, HI)
    split(NA, 5, HI)
    arrive(NB, 2, HI)
    split(NB, 2, HI)
    product(2, 0)
    finish([(7, 0)])
    arrive(NB, 3, LO)
    move(UP, NB, 3, LO)
    arrive(NB, 5, LO)
    split(NB, 3, LO)
    split(NB, 5, LO)
    arrive(NB, 5, HI)
    move(DOWN, NB, 5, HI)
    split(NB, 5, HI)
    product(5, 0)
    finish([(2, 0)])
    for h in range(2):
        tile_copies[h].wait_recv()
        split_tile(1, h)
    for s in (0, 1, 7):
        product(s, 1)
    finish([(5, 0), (0, 1), (1, 1), (7, 1)])
    for s in (2, 5):
        product(s, 1)
    arrive(NA, 4, LO)
    arrive(NA, 4, HI)
    split(NA, 4, LO)
    split(NA, 4, HI)
    arrive(NB, 3, HI)
    split(NB, 3, HI)
    product(3, 0)
    product(3, 1)
    finish([(2, 1), (5, 1), (3, 0), (3, 1)])
    for h in (LO, HI):
        arrive(NB, 4, h)
        split(NB, 4, h)
    product(4, 0)
    product(4, 1)
    arrive(NB, 6, HI)
    split(NB, 6, HI)
    product(6, 0)
    product(6, 1)
    finish([(4, 0), (4, 1), (6, 0), (6, 1)])

    s_mine = (z - g + ZN) % ZN

    def received(p, side, w):
        slot = p * 6 + side * 2 + w
        pltpu.make_async_remote_copy(
            src_ref=csum.at[0], dst_ref=dst.at[slot],
            send_sem=xsend.at[0], recv_sem=rrecv.at[slot],
            device_id=dev(g_sib, m), device_id_type=MESH,
        ).wait_recv()

    def sums(p):
        own = s_mine * 2 + p
        for side in (0, 2):
            for w in range(2):
                received(p, side, w)
        received(p, 1, 1 - core)
        other = 1 - core
        return (
            dst[p * 6 + core] + dst[p * 6 + 4 + core] + csum[own],
            dst[p * 6 + other] + dst[p * 6 + 4 + other] + dst[p * 6 + 2 + other],
        )

    across, behind = sums(1)
    ybuf[core] = across
    ybuf[1 - core] = behind
    to_pair = pltpu.make_async_remote_copy(
        src_ref=ybuf, dst_ref=fin, send_sem=ysend, recv_sem=yrecv,
        device_id=dev(g, m_pair), device_id_type=MESH,
    )
    to_pair.start()

    def keep(row_y, v):
        v = v * v
        stage[row_y] = v
        return jnp.sum(v.reshape(ROWS // 8, 8, TILE), axis=0)

    turn = 3 - 2 * y
    mine, theirs = sums(0)
    total = keep(y + core * turn, mine) + keep(y + (1 - core) * turn, theirs)
    to_pair.wait()
    total += keep(pair_y, fin[0]) + keep(3 - pair_y, fin[1])
    sq[...] = total

    def square_copy(d):
        return pltpu.make_async_remote_copy(
            src_ref=sq, dst_ref=sq_all.at[d - 1], send_sem=qsend.at[d - 1], recv_sem=qrecv.at[d - 1],
            device_id=dev((g + d) % GN, m), device_id_type=MESH,
        )

    for d in range(1, GN):
        square_copy(d).start()
    for d in range(1, GN):
        square_copy(d).wait_recv()
        total += sq_all[d - 1]
    means = jnp.sum(total, axis=0, keepdims=True) / WROWS
    for row_y in range(YN):
        out[pl.ds(row_y * ROWS, ROWS), :] = stage[row_y] / means

    for copy in started:
        copy.wait_send()
    for copy in tile_copies:
        copy.wait_send()
    for s in range(8):
        xt, ct, dx = place(s)
        for p in range(2):
            sibling(s * 2 + p).wait_send()

            @pl.when((dx != 0) | (ct != core))
            def _():
                to_mid(s * 2 + p).wait_send()

    for d in range(1, GN):
        square_copy(d).wait_send()


def per_device(slab, tiles, slot_rows):
    dma = pltpu.SemaphoreType.DMA
    return pl.pallas_call(
        body,
        out_shape=jax.ShapeDtypeStruct((256, TILE), F32),
        in_specs=[
            pl.BlockSpec(memory_space=pltpu.HBM),
            pl.BlockSpec(memory_space=pltpu.HBM),
            pl.BlockSpec(memory_space=pltpu.SMEM),
        ],
        out_specs=pl.BlockSpec(memory_space=pltpu.VMEM),
        scratch_shapes=[
            pltpu.VMEM((2, 8, ROWS, KCOLS), F32),
            pltpu.VMEM((2, 2 * TILE, TILE), F32),
            pltpu.VMEM((4, TILE, TILE), BF16),
            pltpu.VMEM((4, TILE, TILE), BF16),
            pltpu.VMEM((32, 2 * ROWS, TILE), BF16),
            pltpu.VMEM((32, 2 * ROWS, TILE), BF16),
            pltpu.VMEM((16, 2, ROWS, TILE), F32),
            pltpu.VMEM((16, ROWS, TILE), F32),
            pltpu.VMEM((16, ROWS, TILE), F32),
            pltpu.VMEM((16, ROWS, TILE), F32),
            pltpu.VMEM((12, ROWS, TILE), F32),
            pltpu.VMEM((2, ROWS, TILE), F32),
            pltpu.VMEM((2, ROWS, TILE), F32),
            pltpu.VMEM((4, ROWS, TILE), F32),
            pltpu.VMEM((8, TILE), F32),
            pltpu.VMEM((GN - 1, 8, TILE), F32),
            dma((2,)),
            dma((32,)),
            dma((2, 8, 2)),
            dma((2,)),
            dma((2,)),
            dma((16,)),
            dma((16,)),
            dma((16,)),
            dma((16,)),
            dma((12,)),
            dma,
            dma,
            dma((GN - 1,)),
            dma((GN - 1,)),
        ],
        compiler_params=pltpu.CompilerParams(
            collective_id=0, has_side_effects=True, vmem_limit_bytes=60 * 1024 * 1024
        ),
        name="expand",
    )(slab, tiles, slot_rows)


def solution(mesh):
    return jax.shard_map(
        per_device,
        mesh=mesh,
        in_specs=(P("mem", "grp"), P("grp", "mem"), P("grp", None)),
        out_specs=P("grp", "mem"),
        check_vma=False,
    )
```

```python
import functools

import jax
import jax.numpy as jnp
from jax import lax
from jax.experimental import pallas as pl
from jax.experimental.pallas import tpu as pltpu
from jax.sharding import PartitionSpec as P

MESH = pl.DeviceIdType.MESH
F32 = jnp.float32
BF16 = jnp.bfloat16

TILE = 512
ROWS = 64
KCOLS = 2048
HALF = 1024
WIDTH = 256
ZN, YN, XN, GN = 8, 4, 4, 8
WROWS = 2048

UP, DOWN, ACROSS = 0, 1, 2
NA, NB = 0, 1
LO, HI = 0, 1


def body(
    slab, tiles, slot_rows, out,
    rows, tile_buf, thi, tlo, xhi, xlo, part, sib, csum, mid, dst, near, ybuf, fin, stage, sq, sq_all,
    load_sem, gsend, grecv, tsend, trecv, dsend, drecv, xsend, mrecv, rrecv, nrecv, ysend, yrecv, qsend, qrecv,
):
    g = lax.axis_index("grp")
    m = lax.axis_index("mem")
    x, core = g // 2, g % 2
    z, y = m // YN, m % YN
    pair_y = y + 1 - 2 * (y % 2)
    m_up = ((z + 1) % ZN) * YN + y
    m_down = ((z + ZN - 1) % ZN) * YN + y
    m_across = z * YN + (3 - y)
    m_pair = z * YN + pair_y
    g_sib = x * 2 + (1 - core)

    def dev(gi, mi):
        return {"grp": gi, "mem": mi}

    load_slab = pltpu.make_async_copy(slab, rows.at[NA, 0], load_sem.at[0])
    load_tiles = pltpu.make_async_copy(tiles, tile_buf.at[0], load_sem.at[1])
    load_slab.start()
    load_tiles.start()

    barrier = pltpu.get_barrier_semaphore()
    for mi in (m_up, m_down, m_across, m_pair):
        pl.semaphore_signal(barrier, inc=1, device_id=dev(g, mi), device_id_type=MESH)
    for d in range(1, GN):
        pl.semaphore_signal(barrier, inc=1, device_id=dev((g + d) % GN, m), device_id_type=MESH)
    pl.semaphore_wait(barrier, 4 + GN - 1)

    started = []

    def piece(w, s, h):
        return rows.at[w, s, :, pl.ds(h * HALF, HALF)]

    def move(way, w, s, h):
        if way == ACROSS:
            target, tw, ts = m_across, NB, s
        elif way == UP:
            target, tw, ts = m_up, w, s + 1
        else:
            target, tw, ts = m_down, w, (s + 7) % 8
        copy = pltpu.make_async_remote_copy(
            src_ref=piece(w, s, h), dst_ref=piece(tw, ts, h),
            send_sem=gsend.at[len(started)], recv_sem=grecv.at[tw, ts, h],
            device_id=dev(g, target), device_id_type=MESH,
        )
        copy.start()
        started.append(copy)

    def split(w, s, h):
        for b in range(2):
            block = s * 4 + h * 2 + b
            v = rows[w, s, :, pl.ds(h * HALF + b * TILE, TILE)]
            top = v.astype(BF16)
            xhi[block, pl.ds(w * ROWS, ROWS), :] = top
            xlo[block, pl.ds(w * ROWS, ROWS), :] = (v - top.astype(F32)).astype(BF16)

    def arrive(w, s, h):
        pltpu.make_async_remote_copy(
            src_ref=piece(w, s, h), dst_ref=piece(w, s, h),
            send_sem=gsend.at[0], recv_sem=grecv.at[w, s, h],
            device_id=dev(g, m_up), device_id_type=MESH,
        ).wait_recv()

    tile_copies = [
        pltpu.make_async_remote_copy(
            src_ref=tile_buf.at[0, :, pl.ds(q * WIDTH, WIDTH)], dst_ref=tile_buf.at[1, :, pl.ds(q * WIDTH, WIDTH)],
            send_sem=tsend.at[q], recv_sem=trecv.at[q],
            device_id=dev(g, m_pair), device_id_type=MESH,
        )
        for q in range(2)
    ]

    def split_tile(c):
        p, q = c // 2, c % 2
        for h in range(2):
            def step(i, carry):
                r = pl.multiple_of(i * 64, 64)
                v = tile_buf[p, pl.ds(h * TILE + r, 64), pl.ds(q * WIDTH, WIDTH)]
                top = v.astype(BF16)
                thi[c * 2 + h, pl.ds(r, 64), :] = top
                tlo[c * 2 + h, pl.ds(r, 64), :] = (v - top.astype(F32)).astype(BF16)
                return carry
            lax.fori_loop(0, TILE // 64, step, 0)

    def product(s, columns):
        for c in columns:
            member = m if c < 2 else m_pair
            u = s * 4 + c
            total = None
            for h in range(2):
                block = s * 4 + jnp.maximum(slot_rows[h, member], 0)
                a, b = xhi[block], xlo[block]
                top, low = thi[c * 2 + h], tlo[c * 2 + h]
                term = (
                    jnp.dot(a, low, preferred_element_type=F32)
                    + jnp.dot(b, top, preferred_element_type=F32)
                    + jnp.dot(a, top, preferred_element_type=F32)
                )
                total = term if total is None else total + term
            part[u] = total.reshape(2, ROWS, WIDTH)
            sibling(u).start()

    def sibling(u):
        return pltpu.make_async_remote_copy(
            src_ref=part.at[u, 1 - core], dst_ref=sib.at[u],
            send_sem=dsend.at[u], recv_sem=drecv.at[u],
            device_id=dev(g_sib, m), device_id_type=MESH,
        )

    def place(s):
        zt = (z - s + ZN) % ZN
        xt, ct = zt // 2, zt % 2
        dx = (xt - x + XN) % XN
        hop = jnp.where(core == 0, 3 - dx, (dx + 3) % 4)
        return xt, ct, hop

    x_next = (x + 1 + 2 * core) % XN

    def to_next(u):
        return pltpu.make_async_remote_copy(
            src_ref=csum.at[u], dst_ref=mid.at[u],
            send_sem=xsend.at[u], recv_sem=mrecv.at[u],
            device_id=dev(x_next * 2 + core, m), device_id_type=MESH,
        )

    def to_end(u, c, ct):
        return pltpu.make_async_remote_copy(
            src_ref=csum.at[u], dst_ref=dst.at[c, core],
            send_sem=xsend.at[u], recv_sem=rrecv.at[c, core],
            device_id=dev(x_next * 2 + ct, m), device_id_type=MESH,
        )

    def to_sibling(u, c):
        return pltpu.make_async_remote_copy(
            src_ref=csum.at[u], dst_ref=near.at[c],
            send_sem=xsend.at[u], recv_sem=nrecv.at[c],
            device_id=dev(g_sib, m), device_id_type=MESH,
        )

    def chip_sum(s, columns):
        xt, ct, hop = place(s)
        for c in columns:
            u = s * 4 + c
            sibling(u).wait_recv()
            csum[u] = part[u, core] + sib[u]

            @pl.when(hop == 0)
            def _():
                to_next(u).start()

            @pl.when((hop == 3) & (ct != core))
            def _():
                to_sibling(u, c).start()

    def chain(s, columns):
        xt, ct, hop = place(s)

        @pl.when((hop == 1) | (hop == 2))
        def _():
            for c in columns:
                u = s * 4 + c
                to_next(u).wait_recv()
                csum[u] = csum[u] + mid[u]

                @pl.when(hop == 1)
                def _():
                    to_next(u).start()

                @pl.when(hop == 2)
                def _():
                    to_end(u, c, ct).start()

    load_slab.wait()
    for h in (LO, HI):
        move(UP, NA, 0, h)
        move(DOWN, NA, 0, h)
        move(ACROSS, NA, 0, h)
    load_tiles.wait()
    for copy in tile_copies:
        copy.start()
    for h in (LO, HI):
        split(NA, 0, h)
    for c in range(2):
        split_tile(c)

    def arrive_near(h, s_up, s_down):
        arrive(NA, s_up, h)
        move(UP, NA, s_up, h)
        arrive(NA, s_down, h)
        move(DOWN, NA, s_down, h)

    first, third, every = (0, 1), (0, 1, 2), (2, 3, 0, 1)
    for h in (LO, HI):
        arrive_near(h, 1, 7)
        move(ACROSS, NA, 1, h)
        move(ACROSS, NA, 7, h)
        split(NA, 1, h)
        split(NA, 7, h)
        arrive(NB, 0, h)
        split(NB, 0, h)
    product(0, first)
    arrive_near(LO, 2, 6)
    arrive(NB, 1, LO)
    move(UP, NB, 1, LO)
    split(NA, 2, LO)
    split(NA, 6, LO)
    split(NB, 1, LO)
    chip_sum(0, first)
    arrive_near(HI, 2, 6)
    move(ACROSS, NA, 2, HI)
    arrive(NB, 7, LO)
    move(DOWN, NB, 7, LO)
    split(NA, 2, HI)
    split(NA, 6, HI)
    split(NB, 7, LO)
    chain(0, first)
    tile_copies[0].wait_recv()
    split_tile(2)
    product(0, (2,))
    arrive(NA, 3, LO)
    arrive(NA, 5, LO)
    split(NA, 3, LO)
    split(NA, 5, LO)
    arrive(NB, 1, HI)
    split(NB, 1, HI)
    product(1, third)
    chip_sum(0, (2,))
    arrive(NB, 2, LO)
    move(UP, NB, 2, LO)
    move(UP, NA, 3, LO)
    arrive(NB, 6, LO)
    move(DOWN, NB, 6, LO)
    split(NB, 2, LO)
    split(NB, 6, LO)
    arrive(NB, 7, HI)
    split(NB, 7, HI)
    product(7, third)
    chip_sum(1, third)
    chain(0, (2,))
    arrive(NA, 3, HI)
    arrive(NA, 5, HI)
    move(ACROSS, NA, 5, HI)
    move(DOWN, NA, 5, HI)
    move(ACROSS, NA, 3, HI)
    move(ACROSS, NA, 6, HI)
    split(NA, 3, HI)
    split(NA, 5, HI)
    arrive(NB, 2, HI)
    split(NB, 2, HI)
    product(2, third)
    chip_sum(7, third)
    chain(1, third)
    arrive(NB, 3, LO)
    move(UP, NB, 3, LO)
    arrive(NB, 5, LO)
    split(NB, 3, LO)
    split(NB, 5, LO)
    tile_copies[1].wait_recv()
    split_tile(3)
    arrive(NB, 5, HI)
    move(DOWN, NB, 5, HI)
    split(NB, 5, HI)
    for s in (0, 1, 7, 2):
        product(s, (3,))
    chip_sum(2, third)
    chain(7, third)
    product(5, every)
    for s in (0, 1, 7, 2):
        chip_sum(s, (3,))
    chain(2, third)
    arrive(NA, 4, LO)
    arrive(NA, 4, HI)
    split(NA, 4, LO)
    split(NA, 4, HI)
    arrive(NB, 3, HI)
    split(NB, 3, HI)
    product(3, every)
    chip_sum(5, every)
    for s in (0, 1, 7, 2):
        chain(s, (3,))
    chip_sum(3, every)
    for h in (LO, HI):
        arrive(NB, 4, h)
        split(NB, 4, h)
    product(4, every)
    chain(5, every)
    arrive(NB, 6, HI)
    split(NB, 6, HI)
    product(6, every)
    chip_sum(4, every)
    chip_sum(6, every)
    chain(3, every)
    chain(4, every)
    chain(6, every)

    s_mine = (z - g + ZN) % ZN

    def received(src, sem):
        pltpu.make_async_remote_copy(
            src_ref=csum.at[0], dst_ref=src, send_sem=xsend.at[0], recv_sem=sem,
            device_id=dev(g_sib, m), device_id_type=MESH,
        ).wait_recv()

    def sums(c):
        for w in range(2):
            received(dst.at[c, w], rrecv.at[c, w])
        received(near.at[c], nrecv.at[c])
        return dst[c, core] + csum[s_mine * 4 + c], dst[c, 1 - core] + near[c]

    to_pair = []
    for q in range(2):
        mine, other = sums(2 + q)
        ybuf[q, core] = mine
        ybuf[q, 1 - core] = other
        copy = pltpu.make_async_remote_copy(
            src_ref=ybuf.at[q], dst_ref=fin.at[q], send_sem=ysend.at[q], recv_sem=yrecv.at[q],
            device_id=dev(g, m_pair), device_id_type=MESH,
        )
        copy.start()
        to_pair.append(copy)

    def keep(row_y, q, v):
        v = v * v
        stage[row_y, :, pl.ds(q * WIDTH, WIDTH)] = v
        return jnp.sum(v.reshape(ROWS // 8, 8, WIDTH), axis=0)

    turn = 3 - 2 * y
    totals = []
    for q in range(2):
        mine, other = sums(q)
        totals.append(keep(y + core * turn, q, mine) + keep(y + (1 - core) * turn, q, other))
    for q in range(2):
        to_pair[q].wait()
        totals[q] += keep(pair_y, q, fin[q, 0]) + keep(3 - pair_y, q, fin[q, 1])
    total = jnp.concatenate(totals, axis=1)
    sq[...] = total

    def square_copy(d):
        return pltpu.make_async_remote_copy(
            src_ref=sq, dst_ref=sq_all.at[d - 1], send_sem=qsend.at[d - 1], recv_sem=qrecv.at[d - 1],
            device_id=dev((g + d) % GN, m), device_id_type=MESH,
        )

    for d in range(1, GN):
        square_copy(d).start()
    for d in range(1, GN):
        square_copy(d).wait_recv()
        total += sq_all[d - 1]
    means = jnp.sum(total, axis=0, keepdims=True) / WROWS
    for row_y in range(YN):
        out[pl.ds(row_y * ROWS, ROWS), :] = stage[row_y] / means

    for copy in started:
        copy.wait_send()
    for copy in tile_copies:
        copy.wait_send()
    for s in range(8):
        xt, ct, hop = place(s)
        for c in range(4):
            sibling(s * 4 + c).wait_send()

        @pl.when((hop != 3) | (ct != core))
        def _():
            for c in range(4):
                to_next(s * 4 + c).wait_send()

    for d in range(1, GN):
        square_copy(d).wait_send()


def per_device(slab, tiles, slot_rows):
    dma = pltpu.SemaphoreType.DMA
    return pl.pallas_call(
        body,
        out_shape=jax.ShapeDtypeStruct((256, TILE), F32),
        in_specs=[
            pl.BlockSpec(memory_space=pltpu.HBM),
            pl.BlockSpec(memory_space=pltpu.HBM),
            pl.BlockSpec(memory_space=pltpu.SMEM),
        ],
        out_specs=pl.BlockSpec(memory_space=pltpu.VMEM),
        scratch_shapes=[
            pltpu.VMEM((2, 8, ROWS, KCOLS), F32),
            pltpu.VMEM((2, 2 * TILE, TILE), F32),
            pltpu.VMEM((8, TILE, WIDTH), BF16),
            pltpu.VMEM((8, TILE, WIDTH), BF16),
            pltpu.VMEM((32, 2 * ROWS, TILE), BF16),
            pltpu.VMEM((32, 2 * ROWS, TILE), BF16),
            pltpu.VMEM((32, 2, ROWS, WIDTH), F32),
            pltpu.VMEM((32, ROWS, WIDTH), F32),
            pltpu.VMEM((32, ROWS, WIDTH), F32),
            pltpu.VMEM((32, ROWS, WIDTH), F32),
            pltpu.VMEM((4, 2, ROWS, WIDTH), F32),
            pltpu.VMEM((4, ROWS, WIDTH), F32),
            pltpu.VMEM((2, 2, ROWS, WIDTH), F32),
            pltpu.VMEM((2, 2, ROWS, WIDTH), F32),
            pltpu.VMEM((4, ROWS, TILE), F32),
            pltpu.VMEM((8, TILE), F32),
            pltpu.VMEM((GN - 1, 8, TILE), F32),
            dma((2,)),
            dma((32,)),
            dma((2, 8, 2)),
            dma((2,)),
            dma((2,)),
            dma((32,)),
            dma((32,)),
            dma((32,)),
            dma((32,)),
            dma((4, 2)),
            dma((4,)),
            dma((2,)),
            dma((2,)),
            dma((GN - 1,)),
            dma((GN - 1,)),
        ],
        compiler_params=pltpu.CompilerParams(
            collective_id=0, has_side_effects=True, vmem_limit_bytes=60 * 1024 * 1024
        ),
        name="expand",
    )(slab, tiles, slot_rows)


def solution(mesh):
    return jax.shard_map(
        per_device,
        mesh=mesh,
        in_specs=(P("mem", "grp"), P("grp", "mem"), P("grp", None)),
        out_specs=P("grp", "mem"),
        check_vma=False,
    )
```

```python
import functools

import jax
import jax.numpy as jnp
from jax import lax
from jax.experimental import pallas as pl
from jax.experimental.pallas import tpu as pltpu
from jax.sharding import PartitionSpec as P

MESH = pl.DeviceIdType.MESH
F32 = jnp.float32
BF16 = jnp.bfloat16

TILE = 512
ROWS = 64
KCOLS = 2048
HALF = 1024
WIDTH = 256
ZN, YN, XN, GN = 8, 4, 4, 8
WROWS = 2048

UP, DOWN, ACROSS = 0, 1, 2
NA, NB = 0, 1
LO, HI = 0, 1


def body(
    slab, tiles, slot_rows, out,
    rows, tile_buf, thi, tlo, xs, part, sib, csum, mid, dst, near, ybuf, fin, stage, sq, sq_all,
    load_sem, gsend, grecv, tsend, trecv, dsend, drecv, xsend, mrecv, rrecv, nrecv, ysend, yrecv, qsend, qrecv,
):
    g = lax.axis_index("grp")
    m = lax.axis_index("mem")
    x, core = g // 2, g % 2
    z, y = m // YN, m % YN
    pair_y = y + 1 - 2 * (y % 2)
    m_up = ((z + 1) % ZN) * YN + y
    m_down = ((z + ZN - 1) % ZN) * YN + y
    m_across = z * YN + (3 - y)
    m_pair = z * YN + pair_y
    g_sib = x * 2 + (1 - core)

    def dev(gi, mi):
        return {"grp": gi, "mem": mi}

    load_slab = pltpu.make_async_copy(slab, rows.at[NA, 0], load_sem.at[0])
    load_tiles = pltpu.make_async_copy(tiles, tile_buf.at[0], load_sem.at[1])
    load_slab.start()
    load_tiles.start()

    barrier = pltpu.get_barrier_semaphore()
    partners = [(g, mi) for mi in (m_up, m_down, m_across, m_pair)] + [(g_sib, m)]
    for xi in ((x + 1) % XN, (x + XN - 1) % XN):
        partners += [(xi * 2, m), (xi * 2 + 1, m)]
    for gi, mi in partners:
        pl.semaphore_signal(barrier, inc=1, device_id=dev(gi, mi), device_id_type=MESH)
    pl.semaphore_wait(barrier, len(partners))

    started = []

    def piece(w, s, h):
        return rows.at[w, s, :, pl.ds(h * HALF, HALF)]

    def move(way, w, s, h):
        if way == ACROSS:
            target, tw, ts = m_across, NB, s
        elif way == UP:
            target, tw, ts = m_up, w, s + 1
        else:
            target, tw, ts = m_down, w, (s + 7) % 8
        copy = pltpu.make_async_remote_copy(
            src_ref=piece(w, s, h), dst_ref=piece(tw, ts, h),
            send_sem=gsend.at[len(started)], recv_sem=grecv.at[tw, ts, h],
            device_id=dev(g, target), device_id_type=MESH,
        )
        copy.start()
        started.append(copy)

    def split(w, s, h):
        for b in range(2):
            block = s * 4 + h * 2 + b
            v = rows[w, s, :, pl.ds(h * HALF + b * TILE, TILE)]
            top = v.astype(BF16)
            xs[w, block, pl.ds(0, ROWS), :] = top
            xs[w, block, pl.ds(ROWS, ROWS), :] = (v - top.astype(F32)).astype(BF16)

    def arrive(w, s, h):
        pltpu.make_async_remote_copy(
            src_ref=piece(w, s, h), dst_ref=piece(w, s, h),
            send_sem=gsend.at[0], recv_sem=grecv.at[w, s, h],
            device_id=dev(g, m_up), device_id_type=MESH,
        ).wait_recv()

    tile_copies = [
        pltpu.make_async_remote_copy(
            src_ref=tile_buf.at[0, :, pl.ds(q * WIDTH, WIDTH)], dst_ref=tile_buf.at[1, :, pl.ds(q * WIDTH, WIDTH)],
            send_sem=tsend.at[q], recv_sem=trecv.at[q],
            device_id=dev(g, m_pair), device_id_type=MESH,
        )
        for q in range(2)
    ]

    def split_tile(c):
        p, q = c // 2, c % 2
        for h in range(2):
            def step(i, carry):
                r = pl.multiple_of(i * 64, 64)
                v = tile_buf[p, pl.ds(h * TILE + r, 64), pl.ds(q * WIDTH, WIDTH)]
                top = v.astype(BF16)
                thi[p * 2 + h, pl.ds(r, 64), pl.ds(q * WIDTH, WIDTH)] = top
                tlo[p * 2 + h, pl.ds(r, 64), pl.ds(q * WIDTH, WIDTH)] = (v - top.astype(F32)).astype(BF16)
                return carry
            lax.fori_loop(0, TILE // 64, step, 0)

    waiting = [[], [], []]

    def product(items, columns):
        member = m if columns[0] < 2 else m_pair
        p = columns[0] // 2
        lanes = pl.ds(columns[0] % 2 * WIDTH, len(columns) * WIDTH)
        sums_of = [None] * len(items)
        for h in range(2):
            block = jnp.maximum(slot_rows[h, member], 0)
            pieces = [xs[w, s * 4 + block] for w, s in items]
            both = jnp.concatenate(pieces, axis=0)
            tops = jnp.concatenate([v[:ROWS] for v in pieces], axis=0)
            wide = jnp.dot(both, thi[p * 2 + h, :, lanes], preferred_element_type=F32)
            low = jnp.dot(tops, tlo[p * 2 + h, :, lanes], preferred_element_type=F32)
            for i in range(len(items)):
                r = 2 * i * ROWS
                term = (wide[r + ROWS : r + 2 * ROWS] + low[i * ROWS : (i + 1) * ROWS]) + wide[r : r + ROWS]
                sums_of[i] = term if sums_of[i] is None else sums_of[i] + term
        for i, (w, s) in enumerate(items):
            for n, c in enumerate(columns):
                part[w, s * 4 + c] = sums_of[i][:, n * WIDTH : (n + 1) * WIDTH]

            @pl.when(core != w)
            def _():
                for c in columns:
                    sibling(w, s * 4 + c).start()

        waiting[0] += [(w, s, columns) for w, s in items]

    def sibling(w, u):
        return pltpu.make_async_remote_copy(
            src_ref=part.at[w, u], dst_ref=sib.at[u],
            send_sem=dsend.at[u], recv_sem=drecv.at[u],
            device_id=dev(g_sib, m), device_id_type=MESH,
        )

    def place(s):
        zt = (z - s + ZN) % ZN
        xt, ct = zt // 2, zt % 2
        dx = (xt - x + XN) % XN
        hop = jnp.where(core == 0, 3 - dx, (dx + 3) % 4)
        return xt, ct, hop

    x_next = (x + 1 + 2 * core) % XN

    def to_next(u):
        return pltpu.make_async_remote_copy(
            src_ref=csum.at[u], dst_ref=mid.at[u],
            send_sem=xsend.at[u], recv_sem=mrecv.at[u],
            device_id=dev(x_next * 2 + core, m), device_id_type=MESH,
        )

    def to_end(u, c, ct):
        return pltpu.make_async_remote_copy(
            src_ref=csum.at[u], dst_ref=dst.at[c, core],
            send_sem=xsend.at[u], recv_sem=rrecv.at[c, core],
            device_id=dev(x_next * 2 + ct, m), device_id_type=MESH,
        )

    def to_sibling(u, c):
        return pltpu.make_async_remote_copy(
            src_ref=csum.at[u], dst_ref=near.at[c],
            send_sem=xsend.at[u], recv_sem=nrecv.at[c],
            device_id=dev(g_sib, m), device_id_type=MESH,
        )

    def chip_sum(w, s, columns):
        xt, ct, hop = place(s)

        @pl.when(core == w)
        def _():
            for c in columns:
                u = s * 4 + c
                sibling(w, u).wait_recv()
                csum[u] = part[w, u] + sib[u]

                @pl.when(hop == 0)
                def _():
                    to_next(u).start()

                @pl.when((hop == 3) & (ct != core))
                def _():
                    to_sibling(u, c).start()

    def chain(step, w, s, columns):
        xt, ct, hop = place(s)

        @pl.when((core == w) & (hop == step))
        def _():
            for c in columns:
                u = s * 4 + c
                to_next(u).wait_recv()
                csum[u] = csum[u] + mid[u]
                if step == 1:
                    to_next(u).start()
                else:
                    to_end(u, c, ct).start()

    def advance():
        ready, once, twice = waiting
        for job in twice:
            chain(2, *job)
        for job in once:
            chain(1, *job)
        for job in ready:
            chip_sum(*job)
        waiting[:] = [[], ready, once]

    load_slab.wait()
    for h in (LO, HI):
        move(UP, NA, 0, h)
        move(DOWN, NA, 0, h)
        move(ACROSS, NA, 0, h)
    load_tiles.wait()
    for copy in tile_copies:
        copy.start()
    for h in (LO, HI):
        split(NA, 0, h)
    for c in range(2):
        split_tile(c)

    def arrive_near(h, s_up, s_down):
        arrive(NA, s_up, h)
        move(UP, NA, s_up, h)
        arrive(NA, s_down, h)
        move(DOWN, NA, s_down, h)

    own, third, fourth, others = (0, 1), (2,), (3,), (2, 3)
    near0, near17, near26, near35, far17 = (
        [(NA, 0), (NB, 0)], [(NA, 1), (NA, 7)], [(NA, 2), (NA, 6)], [(NA, 3), (NA, 5)], [(NB, 1), (NB, 7)]
    )
    for h in (LO, HI):
        arrive_near(h, 1, 7)
        move(ACROSS, NA, 1, h)
        move(ACROSS, NA, 7, h)
        split(NA, 1, h)
        split(NA, 7, h)
        arrive(NB, 0, h)
        split(NB, 0, h)
    product(near0, own)
    product(near17, own)
    arrive_near(LO, 2, 6)
    arrive(NB, 1, LO)
    move(UP, NB, 1, LO)
    split(NA, 2, LO)
    split(NA, 6, LO)
    split(NB, 1, LO)
    advance()
    arrive(NA, 2, HI)
    move(UP, NA, 2, HI)
    move(ACROSS, NA, 2, HI)
    arrive(NB, 7, LO)
    move(DOWN, NB, 7, LO)
    arrive(NA, 6, HI)
    move(DOWN, NA, 6, HI)
    split(NA, 2, HI)
    split(NA, 6, HI)
    split(NB, 7, LO)
    advance()
    product(near26, own)
    tile_copies[0].wait_recv()
    split_tile(2)
    for items in (near0, near17, near26):
        product(items, third)
    arrive(NA, 3, LO)
    arrive(NA, 5, LO)
    advance()
    split(NA, 3, LO)
    split(NA, 5, LO)
    arrive(NB, 1, HI)
    split(NB, 1, HI)
    arrive(NB, 2, LO)
    move(UP, NB, 2, LO)
    move(UP, NA, 3, LO)
    arrive(NB, 6, LO)
    move(DOWN, NB, 6, LO)
    advance()
    split(NB, 2, LO)
    split(NB, 6, LO)
    arrive(NB, 7, HI)
    split(NB, 7, HI)
    product(far17, own)
    product(far17, third)
    arrive(NA, 3, HI)
    arrive(NA, 5, HI)
    move(ACROSS, NA, 5, HI)
    move(DOWN, NA, 5, HI)
    move(ACROSS, NA, 3, HI)
    move(ACROSS, NA, 6, HI)
    advance()
    split(NA, 3, HI)
    split(NA, 5, HI)
    product(near35, own)
    product(near35, third)
    arrive(NB, 2, HI)
    split(NB, 2, HI)
    arrive(NB, 3, LO)
    move(UP, NB, 3, LO)
    advance()
    arrive(NB, 5, LO)
    split(NB, 3, LO)
    split(NB, 5, LO)
    tile_copies[1].wait_recv()
    split_tile(3)
    for items in (near0, near17, near26):
        product(items, fourth)
    arrive(NB, 5, HI)
    move(DOWN, NB, 5, HI)
    advance()
    split(NB, 5, HI)
    for items in (far17, near35):
        product(items, fourth)
    product([(NB, 2), (NB, 5)], others)
    product([(NB, 2), (NB, 5)], own)
    arrive(NA, 4, LO)
    arrive(NA, 4, HI)
    split(NA, 4, LO)
    split(NA, 4, HI)
    arrive(NB, 3, HI)
    split(NB, 3, HI)
    advance()
    product([(NA, 4), (NB, 3)], others)
    product([(NA, 4), (NB, 3)], own)
    advance()
    for h in (LO, HI):
        arrive(NB, 4, h)
        split(NB, 4, h)
    product([(NB, 4)], others)
    product([(NB, 4)], own)
    advance()
    arrive(NB, 6, HI)
    split(NB, 6, HI)
    product([(NB, 6)], others)
    product([(NB, 6)], own)
    advance()
    advance()
    advance()

    s_mine = (z - g + ZN) % ZN

    def received(src, sem):
        pltpu.make_async_remote_copy(
            src_ref=csum.at[0], dst_ref=src, send_sem=xsend.at[0], recv_sem=sem,
            device_id=dev(g_sib, m), device_id_type=MESH,
        ).wait_recv()

    def sums(c):
        for w in range(2):
            received(dst.at[c, w], rrecv.at[c, w])
        received(near.at[c], nrecv.at[c])
        return dst[c, core] + csum[s_mine * 4 + c], dst[c, 1 - core] + near[c]

    to_pair = []

    def squares(a, b):
        return jnp.sum(a * a, axis=0, keepdims=True) + jnp.sum(b * b, axis=0, keepdims=True)

    def square_copy(n):
        if n < GN - 1:
            src, target = sq.at[0], dev((g + n + 1) % GN, m)
        else:
            src, target = sq.at[1], dev((g + n + 1) % GN, m_pair)
        return pltpu.make_async_remote_copy(
            src_ref=src, dst_ref=sq_all.at[n], send_sem=qsend.at[n], recv_sem=qrecv.at[n],
            device_id=target, device_id_type=MESH,
        )

    for q in range(2):
        mine, other = sums(2 + q)
        ybuf[q, core] = mine
        ybuf[q, 1 - core] = other
        copy = pltpu.make_async_remote_copy(
            src_ref=ybuf.at[q], dst_ref=fin.at[q], send_sem=ysend.at[q], recv_sem=yrecv.at[q],
            device_id=dev(g, m_pair), device_id_type=MESH,
        )
        copy.start()
        to_pair.append(copy)
        sq[1, :, pl.ds(q * WIDTH, WIDTH)] = squares(mine, other)
    for n in range(GN - 1, 2 * GN - 1):
        square_copy(n).start()

    turn = 3 - 2 * y
    totals = []
    for q in range(2):
        mine, other = sums(q)
        stage[y + core * turn, :, pl.ds(q * WIDTH, WIDTH)] = mine * mine
        stage[y + (1 - core) * turn, :, pl.ds(q * WIDTH, WIDTH)] = other * other
        totals.append(squares(mine, other))
    total = jnp.concatenate(totals, axis=1)
    sq[0] = total
    for n in range(GN - 1):
        square_copy(n).start()
    for copy in started:
        copy.wait_send()
    for copy in tile_copies:
        copy.wait_send()
    for s in range(8):
        xt, ct, hop = place(s)
        for c in range(4):
            sibling(0, s * 4 + c).wait_send()

        @pl.when((hop != 3) | (ct != core))
        def _():
            for c in range(4):
                to_next(s * 4 + c).wait_send()

    for n in range(2 * GN - 1):
        square_copy(n).wait_recv()
        total += sq_all[n]
    means = total / WROWS
    for q in range(2):
        to_pair[q].wait()
        for w, row_y in enumerate((pair_y, 3 - pair_y)):
            v = fin[q, w]
            stage[row_y, :, pl.ds(q * WIDTH, WIDTH)] = v * v
    for row_y in range(YN):
        out[pl.ds(row_y * ROWS, ROWS), :] = stage[row_y] / means
    for n in range(2 * GN - 1):
        square_copy(n).wait_send()


def per_device(slab, tiles, slot_rows):
    dma = pltpu.SemaphoreType.DMA
    return pl.pallas_call(
        body,
        out_shape=jax.ShapeDtypeStruct((256, TILE), F32),
        in_specs=[
            pl.BlockSpec(memory_space=pltpu.HBM),
            pl.BlockSpec(memory_space=pltpu.HBM),
            pl.BlockSpec(memory_space=pltpu.SMEM),
        ],
        out_specs=pl.BlockSpec(memory_space=pltpu.VMEM),
        scratch_shapes=[
            pltpu.VMEM((2, 8, ROWS, KCOLS), F32),
            pltpu.VMEM((2, 2 * TILE, TILE), F32),
            pltpu.VMEM((4, TILE, TILE), BF16),
            pltpu.VMEM((4, TILE, TILE), BF16),
            pltpu.VMEM((2, 32, 2 * ROWS, TILE), BF16),
            pltpu.VMEM((2, 32, ROWS, WIDTH), F32),
            pltpu.VMEM((32, ROWS, WIDTH), F32),
            pltpu.VMEM((32, ROWS, WIDTH), F32),
            pltpu.VMEM((32, ROWS, WIDTH), F32),
            pltpu.VMEM((4, 2, ROWS, WIDTH), F32),
            pltpu.VMEM((4, ROWS, WIDTH), F32),
            pltpu.VMEM((2, 2, ROWS, WIDTH), F32),
            pltpu.VMEM((2, 2, ROWS, WIDTH), F32),
            pltpu.VMEM((4, ROWS, TILE), F32),
            pltpu.VMEM((2, 1, TILE), F32),
            pltpu.VMEM((2 * GN - 1, 1, TILE), F32),
            dma((2,)),
            dma((32,)),
            dma((2, 8, 2)),
            dma((2,)),
            dma((2,)),
            dma((32,)),
            dma((32,)),
            dma((32,)),
            dma((32,)),
            dma((4, 2)),
            dma((4,)),
            dma((2,)),
            dma((2,)),
            dma((2 * GN - 1,)),
            dma((2 * GN - 1,)),
        ],
        compiler_params=pltpu.CompilerParams(
            collective_id=0, has_side_effects=True, vmem_limit_bytes=60 * 1024 * 1024
        ),
        name="expand",
    )(slab, tiles, slot_rows)


def solution(mesh):
    return jax.shard_map(
        per_device,
        mesh=mesh,
        in_specs=(P("mem", "grp"), P("grp", "mem"), P("grp", None)),
        out_specs=P("grp", "mem"),
        check_vma=False,
    )
```

```python
import functools

import jax
import jax.numpy as jnp
from jax import lax
from jax.experimental import pallas as pl
from jax.experimental.pallas import tpu as pltpu
from jax.sharding import PartitionSpec as P

MESH = pl.DeviceIdType.MESH
F32 = jnp.float32
BF16 = jnp.bfloat16

TILE = 512
ROWS = 64
KCOLS = 2048
HALF = 1024
WIDTH = 384
UNITS = ((0, 256), (256, 256), (0, 384), (384, 128))
ZN, YN, XN, GN = 8, 4, 4, 8
WROWS = 2048

UP, DOWN, ACROSS = 0, 1, 2
NA, NB = 0, 1
LO, HI = 0, 1


def body(
    slab, tiles, slot_rows, out,
    rows, tile_buf, thi, tlo, xs, part, sib, csum, mid, dst, near, ybuf, fin, stage, sq, sq_all,
    load_sem, gsend, grecv, tsend, trecv, dsend, drecv, xsend, mrecv, rrecv, nrecv, ysend, yrecv, qsend, qrecv, osem,
):
    g = lax.axis_index("grp")
    m = lax.axis_index("mem")
    x, core = g // 2, g % 2
    z, y = m // YN, m % YN
    pair_y = y + 1 - 2 * (y % 2)
    m_up = ((z + 1) % ZN) * YN + y
    m_down = ((z + ZN - 1) % ZN) * YN + y
    m_across = z * YN + (3 - y)
    m_pair = z * YN + pair_y
    g_sib = x * 2 + (1 - core)

    def dev(gi, mi):
        return {"grp": gi, "mem": mi}

    load_slab = pltpu.make_async_copy(slab, rows.at[0], load_sem.at[0])
    load_tiles = pltpu.make_async_copy(tiles, tile_buf.at[0], load_sem.at[1])
    load_slab.start()
    load_tiles.start()

    barrier = pltpu.get_barrier_semaphore()
    partners = [(g, mi) for mi in (m_up, m_down, m_across, m_pair)] + [(g_sib, m)]
    for xi in ((x + 1) % XN, (x + XN - 1) % XN):
        partners += [(xi * 2, m), (xi * 2 + 1, m)]
    for gi, mi in partners:
        pl.semaphore_signal(barrier, inc=1, device_id=dev(gi, mi), device_id_type=MESH)
    pl.semaphore_wait(barrier, len(partners))

    def piece(w, s, h):
        return rows.at[w * 8 + s, :, pl.ds(h * HALF, HALF)]

    def move(way, w, s, h):
        if way == ACROSS:
            target, tw, ts = m_across, NB, s
        elif way == UP:
            target, tw, ts = m_up, w, s + 1
        else:
            target, tw, ts = m_down, w, (s + 7) % 8
        copy = pltpu.make_async_remote_copy(
            src_ref=piece(w, s, h), dst_ref=piece(tw, ts, h),
            send_sem=gsend, recv_sem=grecv.at[tw, ts, h],
            device_id=dev(g, target), device_id_type=MESH,
        )
        copy.start()

    def split(w, s, h):
        for b in range(2):
            block = s * 4 + h * 2 + b
            v = rows[w * 8 + s, :, pl.ds(h * HALF + b * TILE, TILE)]
            top = v.astype(BF16)
            xs[w, block, pl.ds(0, ROWS), :] = top
            xs[w, block, pl.ds(ROWS, ROWS), :] = (v - top.astype(F32)).astype(BF16)

    def arrive(w, s, h):
        pltpu.make_async_remote_copy(
            src_ref=piece(w, s, h), dst_ref=piece(w, s, h),
            send_sem=gsend, recv_sem=grecv.at[w, s, h],
            device_id=dev(g, m_up), device_id_type=MESH,
        ).wait_recv()

    tile_copies = [
        pltpu.make_async_remote_copy(
            src_ref=tile_buf.at[0, :, pl.ds(*UNITS[2 + q])], dst_ref=tile_buf.at[1, :, pl.ds(*UNITS[2 + q])],
            send_sem=tsend, recv_sem=trecv.at[q],
            device_id=dev(g, m_pair), device_id_type=MESH,
        )
        for q in range(2)
    ]

    def split_tile(c):
        p, lanes = c // 2, pl.ds(*UNITS[c])
        for h in range(2):
            def step(i, carry):
                r = pl.multiple_of(i * 64, 64)
                v = tile_buf[p, pl.ds(h * TILE + r, 64), lanes]
                top = v.astype(BF16)
                thi[p * 2 + h, pl.ds(r, 64), lanes] = top
                tlo[p * 2 + h, pl.ds(r, 64), lanes] = (v - top.astype(F32)).astype(BF16)
                return carry
            lax.fori_loop(0, TILE // 64, step, 0)

    waiting = [[], [], []]

    def product(items, columns):
        member = m if columns[0] < 2 else m_pair
        p = columns[0] // 2
        first = UNITS[columns[0]][0]
        lanes = pl.ds(first, sum(UNITS[c][1] for c in columns))
        sums_of = [None] * len(items)
        for h in range(2):
            block = jnp.maximum(slot_rows[h, member], 0)
            pieces = [xs[w, s * 4 + block] for w, s in items]
            both = jnp.concatenate(pieces, axis=0)
            tops = jnp.concatenate([v[:ROWS] for v in pieces], axis=0)
            wide = jnp.dot(both, thi[p * 2 + h, :, lanes], preferred_element_type=F32)
            low = jnp.dot(tops, tlo[p * 2 + h, :, lanes], preferred_element_type=F32)
            for i in range(len(items)):
                r = 2 * i * ROWS
                term = (wide[r + ROWS : r + 2 * ROWS] + low[i * ROWS : (i + 1) * ROWS]) + wide[r : r + ROWS]
                sums_of[i] = term if sums_of[i] is None else sums_of[i] + term
        for i, (w, s) in enumerate(items):
            for c in columns:
                start, wide = UNITS[c]
                part[w, s * 4 + c, :, pl.ds(0, wide)] = sums_of[i][:, start - first : start - first + wide]

            for owner in range(2):
                theirs = [c for c in columns if (c + w) % 2 == owner]
                if theirs:
                    @pl.when(core != owner)
                    def _():
                        for c in theirs:
                            sibling(w, s, c).start()

        waiting[0] += [(w, s, columns) for w, s in items]

    def unit(w, s, c):
        return (w * 8 + s) * 2 + c // 2

    def cut(c):
        return pl.ds(0, UNITS[c][1])

    def sibling(w, s, c):
        u = unit(w, s, c)
        return pltpu.make_async_remote_copy(
            src_ref=part.at[w, s * 4 + c, :, cut(c)], dst_ref=sib.at[u, :, cut(c)],
            send_sem=dsend, recv_sem=drecv.at[u],
            device_id=dev(g_sib, m), device_id_type=MESH,
        )

    def place(s):
        zt = (z - s + ZN) % ZN
        xt, ct = zt // 2, zt % 2
        dx = (xt - x + XN) % XN
        hop = jnp.where(core == 0, 3 - dx, (dx + 3) % 4)
        return xt, ct, hop

    x_next = (x + 1 + 2 * core) % XN

    def to_next(u, c):
        return pltpu.make_async_remote_copy(
            src_ref=csum.at[u, :, cut(c)], dst_ref=mid.at[u, :, cut(c)],
            send_sem=xsend, recv_sem=mrecv.at[u],
            device_id=dev(x_next * 2 + core, m), device_id_type=MESH,
        )

    def to_end(u, w, c, ct):
        return pltpu.make_async_remote_copy(
            src_ref=csum.at[u, :, cut(c)], dst_ref=dst.at[c, w, :, cut(c)],
            send_sem=xsend, recv_sem=rrecv.at[c, w],
            device_id=dev(x_next * 2 + ct, m), device_id_type=MESH,
        )

    def to_sibling(u, w, c):
        return pltpu.make_async_remote_copy(
            src_ref=csum.at[u, :, cut(c)], dst_ref=near.at[c, w, :, cut(c)],
            send_sem=xsend, recv_sem=nrecv.at[c, w],
            device_id=dev(g_sib, m), device_id_type=MESH,
        )

    def chip_sum(w, s, columns):
        xt, ct, hop = place(s)
        for owner in range(2):
            mine = [c for c in columns if (c + w) % 2 == owner]
            if not mine:
                continue

            @pl.when(core == owner)
            def _():
                for c in mine:
                    u = unit(w, s, c)
                    sibling(w, s, c).wait_recv()
                    csum[u, :, cut(c)] = part[w, s * 4 + c, :, cut(c)] + sib[u, :, cut(c)]

                    @pl.when(hop == 0)
                    def _():
                        to_next(u, c).start()

                    @pl.when((hop == 3) & (ct != core))
                    def _():
                        to_sibling(u, w, c).start()

    def chain(step, w, s, columns):
        xt, ct, hop = place(s)
        for owner in range(2):
            mine = [c for c in columns if (c + w) % 2 == owner]
            if not mine:
                continue

            @pl.when((core == owner) & (hop == step))
            def _():
                for c in mine:
                    u = unit(w, s, c)
                    to_next(u, c).wait_recv()
                    csum[u, :, cut(c)] = csum[u, :, cut(c)] + mid[u, :, cut(c)]
                    if step == 1:
                        to_next(u, c).start()
                    else:
                        to_end(u, w, c, ct).start()

    def advance():
        ready, once, twice = waiting
        for job in twice:
            chain(2, *job)
        for job in once:
            chain(1, *job)
        for job in ready:
            chip_sum(*job)
        waiting[:] = [[], ready, once]

    load_slab.wait()
    for h in (LO, HI):
        move(UP, NA, 0, h)
        move(DOWN, NA, 0, h)
        move(ACROSS, NA, 0, h)
    load_tiles.wait()
    for copy in tile_copies:
        copy.start()
    for h in (LO, HI):
        split(NA, 0, h)
    for c in range(2):
        split_tile(c)

    def arrive_near(h, s_up, s_down):
        arrive(NA, s_up, h)
        move(UP, NA, s_up, h)
        arrive(NA, s_down, h)
        move(DOWN, NA, s_down, h)

    own, third, fourth, others = (0, 1), (2,), (3,), (2, 3)
    near0, near17, near26, near35, far17 = (
        [(NA, 0), (NB, 0)], [(NA, 1), (NA, 7)], [(NA, 2), (NA, 6)], [(NA, 3), (NA, 5)], [(NB, 1), (NB, 7)]
    )
    for h in (LO, HI):
        arrive_near(h, 1, 7)
        move(ACROSS, NA, 1, h)
        move(ACROSS, NA, 7, h)
        split(NA, 1, h)
        split(NA, 7, h)
        arrive(NB, 0, h)
        split(NB, 0, h)
    product(near0, own)
    product(near17, own)
    arrive_near(LO, 2, 6)
    arrive(NB, 1, LO)
    move(UP, NB, 1, LO)
    split(NA, 2, LO)
    split(NA, 6, LO)
    split(NB, 1, LO)
    advance()
    arrive(NA, 2, HI)
    move(UP, NA, 2, HI)
    move(ACROSS, NA, 2, HI)
    arrive(NB, 7, LO)
    move(DOWN, NB, 7, LO)
    arrive(NA, 6, HI)
    move(DOWN, NA, 6, HI)
    split(NA, 2, HI)
    split(NA, 6, HI)
    split(NB, 7, LO)
    advance()
    product(near26, own)
    arrive(NA, 3, LO)
    arrive(NA, 5, LO)
    advance()
    split(NA, 3, LO)
    split(NA, 5, LO)
    arrive(NB, 1, HI)
    split(NB, 1, HI)
    arrive(NB, 2, LO)
    move(UP, NB, 2, LO)
    move(UP, NA, 3, LO)
    arrive(NB, 6, LO)
    move(DOWN, NB, 6, LO)
    advance()
    split(NB, 2, LO)
    split(NB, 6, LO)
    arrive(NB, 7, HI)
    split(NB, 7, HI)
    product(far17, own)
    tile_copies[0].wait_recv()
    split_tile(2)
    for items in (near0, near17, near26, far17):
        product(items, third)
    arrive(NA, 3, HI)
    arrive(NA, 5, HI)
    move(ACROSS, NA, 5, HI)
    move(DOWN, NA, 5, HI)
    move(ACROSS, NA, 3, HI)
    move(ACROSS, NA, 6, HI)
    advance()
    split(NA, 3, HI)
    split(NA, 5, HI)
    product(near35, own)
    product(near35, third)
    arrive(NB, 2, HI)
    split(NB, 2, HI)
    arrive(NB, 3, LO)
    move(UP, NB, 3, LO)
    advance()
    arrive(NB, 5, LO)
    split(NB, 3, LO)
    split(NB, 5, LO)
    tile_copies[1].wait_recv()
    split_tile(3)
    for items in (near0, near17, near26):
        product(items, fourth)
    arrive(NB, 5, HI)
    move(DOWN, NB, 5, HI)
    advance()
    split(NB, 5, HI)
    for items in (far17, near35):
        product(items, fourth)
    product([(NB, 2), (NB, 5)], others)
    product([(NB, 2), (NB, 5)], own)
    arrive(NA, 4, LO)
    arrive(NA, 4, HI)
    split(NA, 4, LO)
    split(NA, 4, HI)
    arrive(NB, 3, HI)
    split(NB, 3, HI)
    product([(NA, 4), (NB, 3)], others)
    product([(NA, 4), (NB, 3)], own)
    advance()
    for h in (LO, HI):
        arrive(NB, 4, h)
        split(NB, 4, h)
    product([(NB, 4)], others)
    product([(NB, 4)], own)
    advance()
    arrive(NB, 6, HI)
    split(NB, 6, HI)
    product([(NB, 6)], others)
    product([(NB, 6)], own)
    advance()
    advance()
    advance()

    s_mine = (z - g + ZN) % ZN

    def received(c, src, sem):
        pltpu.make_async_remote_copy(
            src_ref=csum.at[0, :, cut(c)], dst_ref=src, send_sem=xsend, recv_sem=sem,
            device_id=dev(g_sib, m), device_id_type=MESH,
        ).wait_recv()

    def sums(c):
        rows_of = []
        for w in range(2):
            received(c, dst.at[c, w, :, cut(c)], rrecv.at[c, w])

            @pl.when(core == (c + w) % 2)
            def _():
                near[c, w, :, cut(c)] = csum[unit(w, s_mine, c), :, cut(c)]

            @pl.when(core != (c + w) % 2)
            def _():
                received(c, near.at[c, w, :, cut(c)], nrecv.at[c, w])

            rows_of.append(dst[c, w, :, cut(c)] + near[c, w, :, cut(c)])
        return rows_of

    to_pair = []

    def squares(a, b):
        return jnp.sum(a * a, axis=0, keepdims=True) + jnp.sum(b * b, axis=0, keepdims=True)

    def square_copy(n):
        if n < GN - 1:
            src, target = sq.at[0], dev((g + n + 1) % GN, m)
        else:
            src, target = sq.at[1], dev((g + n + 1) % GN, m_pair)
        return pltpu.make_async_remote_copy(
            src_ref=src, dst_ref=sq_all.at[n], send_sem=qsend, recv_sem=qrecv,
            device_id=target, device_id_type=MESH,
        )

    for q in range(2):
        mine, other = sums(2 + q)
        ybuf[q, 0, :, cut(2 + q)] = mine
        ybuf[q, 1, :, cut(2 + q)] = other
        copy = pltpu.make_async_remote_copy(
            src_ref=ybuf.at[q, :, :, cut(2 + q)], dst_ref=fin.at[q, :, :, cut(2 + q)], send_sem=ysend, recv_sem=yrecv.at[q],
            device_id=dev(g, m_pair), device_id_type=MESH,
        )
        copy.start()
        to_pair.append(copy)
        sq[1, :, pl.ds(*UNITS[2 + q])] = squares(mine, other)
    for n in range(GN - 1, 2 * GN - 1):
        square_copy(n).start()

    totals = []
    for q in range(2):
        mine, other = sums(q)
        stage[y, :, pl.ds(*UNITS[q])] = mine * mine
        stage[3 - y, :, pl.ds(*UNITS[q])] = other * other
        totals.append(squares(mine, other))
    total = jnp.concatenate(totals, axis=1)
    sq[0] = total
    for n in range(GN - 1):
        square_copy(n).start()
    def all_sent(sem, ref):
        pltpu.make_async_remote_copy(
            src_ref=ref, dst_ref=ref, send_sem=sem, recv_sem=sem,
            device_id=dev(g_sib, m), device_id_type=MESH,
        ).wait_send()

    all_sent(gsend, rows.at[pl.ds(0, 15)])
    all_sent(tsend, tile_buf.at[0])
    all_sent(dsend, rows.at[pl.ds(0, 4)])
    all_sent(xsend, rows.at[pl.ds(0, 7), :, pl.ds(0, HALF)])
    all_sent(ysend, stage.at[pl.ds(0, 2)])

    pltpu.make_async_remote_copy(
        src_ref=sq_all, dst_ref=sq_all, send_sem=qsend, recv_sem=qrecv,
        device_id=dev(g_sib, m), device_id_type=MESH,
    ).wait()
    for n in range(2 * GN - 1):
        total += sq_all[n]
    means = total / WROWS
    for q in range(2):
        to_pair[q].wait_recv()
        for w, row_y in enumerate((pair_y, 3 - pair_y)):
            v = fin[q, w, :, cut(2 + q)]
            stage[row_y, :, pl.ds(*UNITS[2 + q])] = v * v
    leaves = []
    for row_y in range(YN):
        stage[row_y] = stage[row_y] / means
        leave = pltpu.make_async_copy(stage.at[row_y], out.at[pl.ds(row_y * ROWS, ROWS), :], osem.at[row_y])
        leave.start()
        leaves.append(leave)
    for leave in leaves:
        leave.wait()


def per_device(slab, tiles, slot_rows):
    dma = pltpu.SemaphoreType.DMA
    return pl.pallas_call(
        body,
        out_shape=jax.ShapeDtypeStruct((256, TILE), F32),
        in_specs=[
            pl.BlockSpec(memory_space=pltpu.HBM),
            pl.BlockSpec(memory_space=pltpu.HBM),
            pl.BlockSpec(memory_space=pltpu.SMEM),
        ],
        out_specs=pl.BlockSpec(memory_space=pltpu.HBM),
        scratch_shapes=[
            pltpu.VMEM((16, ROWS, KCOLS), F32),
            pltpu.VMEM((2, 2 * TILE, TILE), F32),
            pltpu.VMEM((4, TILE, TILE), BF16),
            pltpu.VMEM((4, TILE, TILE), BF16),
            pltpu.VMEM((2, 32, 2 * ROWS, TILE), BF16),
            pltpu.VMEM((2, 32, ROWS, WIDTH), F32),
            pltpu.VMEM((32, ROWS, WIDTH), F32),
            pltpu.VMEM((32, ROWS, WIDTH), F32),
            pltpu.VMEM((32, ROWS, WIDTH), F32),
            pltpu.VMEM((4, 2, ROWS, WIDTH), F32),
            pltpu.VMEM((4, 2, ROWS, WIDTH), F32),
            pltpu.VMEM((2, 2, ROWS, WIDTH), F32),
            pltpu.VMEM((2, 2, ROWS, WIDTH), F32),
            pltpu.VMEM((4, ROWS, TILE), F32),
            pltpu.VMEM((2, 1, TILE), F32),
            pltpu.VMEM((2 * GN - 1, 1, TILE), F32),
            dma((2,)),
            dma,
            dma((2, 8, 2)),
            dma,
            dma((2,)),
            dma,
            dma((32,)),
            dma,
            dma((32,)),
            dma((4, 2)),
            dma((4, 2)),
            dma,
            dma((2,)),
            dma,
            dma,
            dma((4,)),
        ],
        compiler_params=pltpu.CompilerParams(
            collective_id=0, has_side_effects=True, vmem_limit_bytes=60 * 1024 * 1024
        ),
        name="expand",
    )(slab, tiles, slot_rows)


def solution(mesh):
    return jax.shard_map(
        per_device,
        mesh=mesh,
        in_specs=(P("mem", "grp"), P("grp", "mem"), P("grp", None)),
        out_specs=P("grp", "mem"),
        check_vma=False,
    )
```

```python
import functools

import jax
import jax.numpy as jnp
from jax import lax
from jax.experimental import pallas as pl
from jax.experimental.pallas import tpu as pltpu
from jax.sharding import PartitionSpec as P

MESH = pl.DeviceIdType.MESH
F32 = jnp.float32
BF16 = jnp.bfloat16

TILE = 512
ROWS = 64
KCOLS = 2048
HALF = 1024
WIDTH = 384
UNITS = ((0, 256), (256, 256), (0, 384), (384, 128))
ZN, YN, XN, GN = 8, 4, 4, 8
WROWS = 2048

UP, DOWN, ACROSS = 0, 1, 2
NA, NB = 0, 1
LO, HI = 0, 1


def body(
    slab, tiles, slot_rows, out,
    rows, tile_buf, thi, tlo, xs, part, sib, csum, mid, dst, near, ybuf, fin, stage, sq, sq_all,
    load_sem, gsend, grecv, tsend, trecv, dsend, drecv, xsend, mrecv, rrecv, nrecv, ysend, yrecv, qsend, qrecv, osem,
):
    g = lax.axis_index("grp")
    m = lax.axis_index("mem")
    x, core = g // 2, g % 2
    z, y = m // YN, m % YN
    pair_y = y + 1 - 2 * (y % 2)
    m_up = ((z + 1) % ZN) * YN + y
    m_down = ((z + ZN - 1) % ZN) * YN + y
    m_across = z * YN + (3 - y)
    m_pair = z * YN + pair_y
    g_sib = x * 2 + (1 - core)

    def dev(gi, mi):
        return {"grp": gi, "mem": mi}

    load_slab = pltpu.make_async_copy(slab, rows.at[0], load_sem.at[0])
    load_tiles = pltpu.make_async_copy(tiles, tile_buf.at[0], load_sem.at[1])
    load_slab.start()
    load_tiles.start()

    barrier = pltpu.get_barrier_semaphore()
    partners = [(g, mi) for mi in (m_up, m_down, m_across, m_pair)] + [(g_sib, m)]
    for xi in ((x + 1) % XN, (x + XN - 1) % XN):
        partners += [(xi * 2, m), (xi * 2 + 1, m)]
    for gi, mi in partners:
        pl.semaphore_signal(barrier, inc=1, device_id=dev(gi, mi), device_id_type=MESH)
    pl.semaphore_wait(barrier, len(partners))

    def piece(w, s, h):
        return rows.at[w * 8 + s, :, pl.ds(h * HALF, HALF)]

    def move(way, w, s, h):
        if way == ACROSS:
            target, tw, ts = m_across, NB, s
        elif way == UP:
            target, tw, ts = m_up, w, s + 1
        else:
            target, tw, ts = m_down, w, (s + 7) % 8
        copy = pltpu.make_async_remote_copy(
            src_ref=piece(w, s, h), dst_ref=piece(tw, ts, h),
            send_sem=gsend, recv_sem=grecv.at[tw, ts, h],
            device_id=dev(g, target), device_id_type=MESH,
        )
        copy.start()

    def split(w, s, h):
        for b in range(2):
            block = s * 4 + h * 2 + b
            v = rows[w * 8 + s, :, pl.ds(h * HALF + b * TILE, TILE)]
            top = v.astype(BF16)
            xs[w, block, pl.ds(0, ROWS), :] = top
            xs[w, block, pl.ds(ROWS, ROWS), :] = (v - top.astype(F32)).astype(BF16)

    def arrive(w, s, h):
        pltpu.make_async_remote_copy(
            src_ref=piece(w, s, h), dst_ref=piece(w, s, h),
            send_sem=gsend, recv_sem=grecv.at[w, s, h],
            device_id=dev(g, m_up), device_id_type=MESH,
        ).wait_recv()

    tile_copies = [
        pltpu.make_async_remote_copy(
            src_ref=tile_buf.at[0, :, pl.ds(*UNITS[2 + q])], dst_ref=tile_buf.at[1, :, pl.ds(*UNITS[2 + q])],
            send_sem=tsend, recv_sem=trecv.at[q],
            device_id=dev(g, m_pair), device_id_type=MESH,
        )
        for q in range(2)
    ]

    def split_tile(c):
        p, lanes = c // 2, pl.ds(*UNITS[c])
        for h in range(2):
            def step(i, carry):
                r = pl.multiple_of(i * 64, 64)
                v = tile_buf[p, pl.ds(h * TILE + r, 64), lanes]
                top = v.astype(BF16)
                thi[p * 2 + h, pl.ds(r, 64), lanes] = top
                tlo[p * 2 + h, pl.ds(r, 64), lanes] = (v - top.astype(F32)).astype(BF16)
                return carry
            lax.fori_loop(0, TILE // 64, step, 0)

    waiting = [[], [], []]

    def product(items, columns):
        member = m if columns[0] < 2 else m_pair
        p = columns[0] // 2
        first = UNITS[columns[0]][0]
        lanes = pl.ds(first, sum(UNITS[c][1] for c in columns))
        sums_of = [None] * len(items)
        for h in range(2):
            block = jnp.maximum(slot_rows[h, member], 0)
            pieces = [xs[w, s * 4 + block] for w, s in items]
            both = jnp.concatenate(pieces, axis=0)
            tops = jnp.concatenate([v[:ROWS] for v in pieces], axis=0)
            wide = jnp.dot(both, thi[p * 2 + h, :, lanes], preferred_element_type=F32)
            low = jnp.dot(tops, tlo[p * 2 + h, :, lanes], preferred_element_type=F32)
            for i in range(len(items)):
                r = 2 * i * ROWS
                term = (wide[r + ROWS : r + 2 * ROWS] + low[i * ROWS : (i + 1) * ROWS]) + wide[r : r + ROWS]
                sums_of[i] = term if sums_of[i] is None else sums_of[i] + term
        for i, (w, s) in enumerate(items):
            for c in columns:
                start, wide = UNITS[c]
                part[w, s * 4 + c, :, pl.ds(0, wide)] = sums_of[i][:, start - first : start - first + wide]

            for owner in range(2):
                theirs = [c for c in columns if (c + w) % 2 == owner]
                if theirs:
                    @pl.when(core != owner)
                    def _():
                        for c in theirs:
                            sibling(w, s, c).start()

        waiting[0] += [(w, s, columns) for w, s in items]

    def unit(w, s, c):
        return (w * 8 + s) * 2 + c // 2

    def cut(c):
        return pl.ds(0, UNITS[c][1])

    def sibling(w, s, c):
        u = unit(w, s, c)
        return pltpu.make_async_remote_copy(
            src_ref=part.at[w, s * 4 + c, :, cut(c)], dst_ref=sib.at[u, :, cut(c)],
            send_sem=dsend, recv_sem=drecv.at[u],
            device_id=dev(g_sib, m), device_id_type=MESH,
        )

    def place(s):
        zt = (z - s + ZN) % ZN
        xt, ct = zt // 2, zt % 2
        dx = (xt - x + XN) % XN
        hop = jnp.where(core == 0, 3 - dx, (dx + 3) % 4)
        return xt, ct, hop

    x_next = (x + 1 + 2 * core) % XN

    def to_next(u, c):
        return pltpu.make_async_remote_copy(
            src_ref=csum.at[u, :, cut(c)], dst_ref=mid.at[u, :, cut(c)],
            send_sem=xsend, recv_sem=mrecv.at[u],
            device_id=dev(x_next * 2 + core, m), device_id_type=MESH,
        )

    def to_end(u, w, c, ct):
        return pltpu.make_async_remote_copy(
            src_ref=csum.at[u, :, cut(c)], dst_ref=dst.at[c, w, :, cut(c)],
            send_sem=xsend, recv_sem=rrecv.at[c, w],
            device_id=dev(x_next * 2 + ct, m), device_id_type=MESH,
        )

    def to_sibling(u, w, c):
        return pltpu.make_async_remote_copy(
            src_ref=csum.at[u, :, cut(c)], dst_ref=near.at[c, w, :, cut(c)],
            send_sem=xsend, recv_sem=nrecv.at[c, w],
            device_id=dev(g_sib, m), device_id_type=MESH,
        )

    def chip_sum(w, s, columns):
        xt, ct, hop = place(s)
        for owner in range(2):
            mine = [c for c in columns if (c + w) % 2 == owner]
            if not mine:
                continue

            @pl.when(core == owner)
            def _():
                for c in mine:
                    u = unit(w, s, c)
                    sibling(w, s, c).wait_recv()
                    csum[u, :, cut(c)] = part[w, s * 4 + c, :, cut(c)] + sib[u, :, cut(c)]

                    @pl.when(hop == 0)
                    def _():
                        to_next(u, c).start()

                    @pl.when((hop == 3) & (ct != core))
                    def _():
                        to_sibling(u, w, c).start()

    def chain(step, w, s, columns):
        xt, ct, hop = place(s)
        for owner in range(2):
            mine = [c for c in columns if (c + w) % 2 == owner]
            if not mine:
                continue

            @pl.when((core == owner) & (hop == step))
            def _():
                for c in mine:
                    u = unit(w, s, c)
                    to_next(u, c).wait_recv()
                    csum[u, :, cut(c)] = csum[u, :, cut(c)] + mid[u, :, cut(c)]
                    if step == 1:
                        to_next(u, c).start()
                    else:
                        to_end(u, w, c, ct).start()

    def advance():
        ready, once, twice = waiting
        for job in twice:
            chain(2, *job)
        for job in once:
            chain(1, *job)
        for job in ready:
            chip_sum(*job)
        waiting[:] = [[], ready, once]

    load_slab.wait()
    for h in (LO, HI):
        move(UP, NA, 0, h)
        move(DOWN, NA, 0, h)
        move(ACROSS, NA, 0, h)
    load_tiles.wait()
    for copy in tile_copies:
        copy.start()
    for h in (LO, HI):
        split(NA, 0, h)
    for c in range(2):
        split_tile(c)

    def arrive_near(h, s_up, s_down):
        arrive(NA, s_up, h)
        move(UP, NA, s_up, h)
        arrive(NA, s_down, h)
        move(DOWN, NA, s_down, h)

    own, third, fourth, others = (0, 1), (2,), (3,), (2, 3)
    near0, near17, near26, near35, far17 = (
        [(NA, 0), (NB, 0)], [(NA, 1), (NA, 7)], [(NA, 2), (NA, 6)], [(NA, 3), (NA, 5)], [(NB, 1), (NB, 7)]
    )
    for h in (LO, HI):
        arrive_near(h, 1, 7)
        move(ACROSS, NA, 1, h)
        move(ACROSS, NA, 7, h)
        split(NA, 1, h)
        split(NA, 7, h)
        arrive(NB, 0, h)
        split(NB, 0, h)
    product(near0, own)
    product(near17, own)
    arrive_near(LO, 2, 6)
    arrive(NB, 1, LO)
    move(UP, NB, 1, LO)
    split(NA, 2, LO)
    split(NA, 6, LO)
    split(NB, 1, LO)
    advance()
    arrive(NA, 2, HI)
    move(UP, NA, 2, HI)
    move(ACROSS, NA, 2, HI)
    arrive(NB, 7, LO)
    move(DOWN, NB, 7, LO)
    arrive(NA, 6, HI)
    move(DOWN, NA, 6, HI)
    split(NA, 2, HI)
    split(NA, 6, HI)
    split(NB, 7, LO)
    advance()
    product(near26, own)
    arrive(NA, 3, LO)
    arrive(NA, 5, LO)
    advance()
    split(NA, 3, LO)
    split(NA, 5, LO)
    arrive(NB, 1, HI)
    split(NB, 1, HI)
    arrive(NB, 2, LO)
    move(UP, NB, 2, LO)
    move(UP, NA, 3, LO)
    arrive(NB, 6, LO)
    move(DOWN, NB, 6, LO)
    advance()
    split(NB, 2, LO)
    split(NB, 6, LO)
    arrive(NB, 7, HI)
    split(NB, 7, HI)
    product(far17, own)
    tile_copies[0].wait_recv()
    split_tile(2)
    for items in (near0, near17, near26, far17):
        product(items, third)
    arrive(NA, 3, HI)
    arrive(NA, 5, HI)
    move(ACROSS, NA, 5, HI)
    move(DOWN, NA, 5, HI)
    move(ACROSS, NA, 3, HI)
    move(ACROSS, NA, 6, HI)
    advance()
    split(NA, 3, HI)
    split(NA, 5, HI)
    product(near35, own)
    product(near35, third)
    arrive(NB, 2, HI)
    split(NB, 2, HI)
    arrive(NB, 3, LO)
    move(UP, NB, 3, LO)
    advance()
    arrive(NB, 5, LO)
    split(NB, 3, LO)
    split(NB, 5, LO)
    tile_copies[1].wait_recv()
    split_tile(3)
    for items in (near0, near17, near26):
        product(items, fourth)
    arrive(NB, 5, HI)
    move(DOWN, NB, 5, HI)
    advance()
    split(NB, 5, HI)
    for items in (far17, near35):
        product(items, fourth)
    product([(NB, 2), (NB, 5)], others)
    product([(NB, 2), (NB, 5)], own)
    arrive(NA, 4, LO)
    arrive(NA, 4, HI)
    split(NA, 4, LO)
    split(NA, 4, HI)
    arrive(NB, 3, HI)
    split(NB, 3, HI)
    product([(NA, 4), (NB, 3)], others)
    product([(NA, 4), (NB, 3)], own)
    advance()
    for h in (LO, HI):
        arrive(NB, 4, h)
        split(NB, 4, h)
    arrive(NB, 6, HI)
    split(NB, 6, HI)
    product([(NB, 4), (NB, 6)], others)
    product([(NB, 4), (NB, 6)], own)
    advance()
    advance()
    advance()

    s_mine = (z - g + ZN) % ZN

    def received(c, src, sem):
        pltpu.make_async_remote_copy(
            src_ref=csum.at[0, :, cut(c)], dst_ref=src, send_sem=xsend, recv_sem=sem,
            device_id=dev(g_sib, m), device_id_type=MESH,
        ).wait_recv()

    def sums(c):
        rows_of = []
        for w in range(2):
            received(c, dst.at[c, w, :, cut(c)], rrecv.at[c, w])

            @pl.when(core == (c + w) % 2)
            def _():
                near[c, w, :, cut(c)] = csum[unit(w, s_mine, c), :, cut(c)]

            @pl.when(core != (c + w) % 2)
            def _():
                received(c, near.at[c, w, :, cut(c)], nrecv.at[c, w])

            rows_of.append(dst[c, w, :, cut(c)] + near[c, w, :, cut(c)])
        return rows_of

    to_pair = []

    def squares(a, b):
        return jnp.sum(a * a, axis=0, keepdims=True) + jnp.sum(b * b, axis=0, keepdims=True)

    def square_copy(n):
        if n < GN - 1:
            src, target = sq.at[0], dev((g + n + 1) % GN, m)
        else:
            src, target = sq.at[1], dev((g + n + 1) % GN, m_pair)
        return pltpu.make_async_remote_copy(
            src_ref=src, dst_ref=sq_all.at[n], send_sem=qsend, recv_sem=qrecv,
            device_id=target, device_id_type=MESH,
        )

    for q in range(2):
        mine, other = sums(2 + q)
        ybuf[q, 0, :, cut(2 + q)] = mine
        ybuf[q, 1, :, cut(2 + q)] = other
        copy = pltpu.make_async_remote_copy(
            src_ref=ybuf.at[q, :, :, cut(2 + q)], dst_ref=fin.at[q, :, :, cut(2 + q)], send_sem=ysend, recv_sem=yrecv.at[q],
            device_id=dev(g, m_pair), device_id_type=MESH,
        )
        copy.start()
        to_pair.append(copy)
        sq[1, :, pl.ds(*UNITS[2 + q])] = squares(mine, other)
    for n in range(GN - 1, 2 * GN - 1):
        square_copy(n).start()

    totals = []
    for q in range(2):
        mine, other = sums(q)
        stage[y, :, pl.ds(*UNITS[q])] = mine * mine
        stage[3 - y, :, pl.ds(*UNITS[q])] = other * other
        totals.append(squares(mine, other))
    total = jnp.concatenate(totals, axis=1)
    sq[0] = total
    for n in range(GN - 1):
        square_copy(n).start()
    def all_sent(sem, ref):
        pltpu.make_async_remote_copy(
            src_ref=ref, dst_ref=ref, send_sem=sem, recv_sem=sem,
            device_id=dev(g_sib, m), device_id_type=MESH,
        ).wait_send()

    all_sent(gsend, rows.at[pl.ds(0, 15)])
    all_sent(tsend, tile_buf.at[0])
    all_sent(dsend, rows.at[pl.ds(0, 4)])
    all_sent(xsend, rows.at[pl.ds(0, 7), :, pl.ds(0, HALF)])
    all_sent(ysend, stage.at[pl.ds(0, 2)])

    pltpu.make_async_remote_copy(
        src_ref=sq_all, dst_ref=sq_all, send_sem=qsend, recv_sem=qrecv,
        device_id=dev(g_sib, m), device_id_type=MESH,
    ).wait()
    for n in range(2 * GN - 1):
        total += sq_all[n]
    means = total / WROWS
    for q in range(2):
        to_pair[q].wait_recv()
        for w, row_y in enumerate((pair_y, 3 - pair_y)):
            v = fin[q, w, :, cut(2 + q)]
            stage[row_y, :, pl.ds(*UNITS[2 + q])] = v * v
    leaves = []
    for row_y in range(YN):
        stage[row_y] = stage[row_y] / means
        leave = pltpu.make_async_copy(stage.at[row_y], out.at[pl.ds(row_y * ROWS, ROWS), :], osem.at[row_y])
        leave.start()
        leaves.append(leave)
    for leave in leaves:
        leave.wait()


def per_device(slab, tiles, slot_rows):
    dma = pltpu.SemaphoreType.DMA
    return pl.pallas_call(
        body,
        out_shape=jax.ShapeDtypeStruct((256, TILE), F32),
        in_specs=[
            pl.BlockSpec(memory_space=pltpu.HBM),
            pl.BlockSpec(memory_space=pltpu.HBM),
            pl.BlockSpec(memory_space=pltpu.SMEM),
        ],
        out_specs=pl.BlockSpec(memory_space=pltpu.HBM),
        scratch_shapes=[
            pltpu.VMEM((16, ROWS, KCOLS), F32),
            pltpu.VMEM((2, 2 * TILE, TILE), F32),
            pltpu.VMEM((4, TILE, TILE), BF16),
            pltpu.VMEM((4, TILE, TILE), BF16),
            pltpu.VMEM((2, 32, 2 * ROWS, TILE), BF16),
            pltpu.VMEM((2, 32, ROWS, WIDTH), F32),
            pltpu.VMEM((32, ROWS, WIDTH), F32),
            pltpu.VMEM((32, ROWS, WIDTH), F32),
            pltpu.VMEM((32, ROWS, WIDTH), F32),
            pltpu.VMEM((4, 2, ROWS, WIDTH), F32),
            pltpu.VMEM((4, 2, ROWS, WIDTH), F32),
            pltpu.VMEM((2, 2, ROWS, WIDTH), F32),
            pltpu.VMEM((2, 2, ROWS, WIDTH), F32),
            pltpu.VMEM((4, ROWS, TILE), F32),
            pltpu.VMEM((2, 1, TILE), F32),
            pltpu.VMEM((2 * GN - 1, 1, TILE), F32),
            dma((2,)),
            dma,
            dma((2, 8, 2)),
            dma,
            dma((2,)),
            dma,
            dma((32,)),
            dma,
            dma((32,)),
            dma((4, 2)),
            dma((4, 2)),
            dma,
            dma((2,)),
            dma,
            dma,
            dma((4,)),
        ],
        compiler_params=pltpu.CompilerParams(
            collective_id=0, has_side_effects=True, vmem_limit_bytes=60 * 1024 * 1024
        ),
        name="expand",
    )(slab, tiles, slot_rows)


def solution(mesh):
    return jax.shard_map(
        per_device,
        mesh=mesh,
        in_specs=(P("mem", "grp"), P("grp", "mem"), P("grp", None)),
        out_specs=P("grp", "mem"),
        check_vma=False,
    )
```
